8 devices in a mesh: replica: 2 (over z, y), data: 4 (over x, core).
Axes of the slice: x: 2, y: 2, z: 1, core: 2. Of those that a mesh axis runs over, the one named last changes fastest.
Arguments:
- x: bfloat16 [4096, 5120], P(('replica', 'data')), parts along dimension 0
- adapter_id: int32 [4096], P(('replica', 'data')), parts along dimension 0
- w_gate: bfloat16 [5120, 13824], replicated
- w_up: bfloat16 [5120, 13824], replicated
- w_down: bfloat16 [13824, 5120], replicated
- a_gate: bfloat16 [64, 5120, 64], P('data')
- b_gate: bfloat16 [64, 64, 13824], P('data')
- a_up: bfloat16 [64, 5120, 64], P('data')
- b_up: bfloat16 [64, 64, 13824], P('data')
- a_down: bfloat16 [64, 13824, 64], P('data')
- b_down: bfloat16 [64, 64, 5120], P('data')
- hot_ids: int32 [4], replicated
- hot_a_gate: bfloat16 [4, 5120, 64], replicated
- hot_b_gate: bfloat16 [4, 64, 13824], replicated
- hot_a_up: bfloat16 [4, 5120, 64], replicated
- hot_b_up: bfloat16 [4, 64, 13824], replicated
- hot_a_down: bfloat16 [4, 13824, 64], replicated
- hot_b_down: bfloat16 [4, 64, 5120], replicated
Outputs:
- output: bfloat16 [4096, 5120], P(('replica', 'data')), parts along dimension 0
There are 2 independent parts. The reference program is written for one: setup_inputs(seed, part) draws one part's arguments, and reference() takes and returns one part's arrays. A program takes and returns all parts, laid end to end along the dimension named above; an argument that names none is the same for every part.
All inputs are finite; a program needn't handle non-finite values.
Results may differ from the reference program's by a relative error of at most 0.00183.
Values are sent between devices in bfloat16 or wider.
A program may use at most 2.25 GiB of HBM per device.

```python
import jax
import jax.numpy as jnp
from jax import lax

GROUP = 4
T_LOC = 512
D = 5120
F = 13824
R = 64
N_LOC = 16
HOT_K = 4
LORA_ALPHA = 32
TOK_BLOCK = 128
TOKENS = GROUP * T_LOC
ADAPTERS = GROUP * N_LOC
CAP = T_LOC // (2 * GROUP)
LORA_SCALE = LORA_ALPHA / R


def draw_hot(hot_key):
    owner_key, local_key = jax.random.split(hot_key)
    hot_owner = jax.random.permutation(owner_key, GROUP)[:HOT_K]
    hot_local = jax.random.randint(local_key, (HOT_K,), 0, N_LOC)
    return hot_owner, hot_local


def draw_ids(id_key, hot_owner, hot_local):
    shift_key, peak_key, count_key, perm_key, cold_key, pick_key = jax.random.split(id_key, 6)
    owners = jnp.arange(GROUP)
    peak_owner = jax.random.randint(peak_key, (), 0, GROUP)
    pop_shift = jnp.where(owners == peak_owner, 0, jax.random.randint(shift_key, (GROUP,), 0, 4))
    cap_upper = jnp.maximum(CAP // (2 ** pop_shift), 1)
    cap_lower = jnp.maximum(cap_upper // 2, 1)
    counts = jax.random.randint(count_key, (GROUP, GROUP), cap_lower[None, :], cap_upper[None, :] + 1)
    counts = jnp.where(owners[None, :] == peak_owner, CAP, counts)
    count_ends = jnp.cumsum(counts, axis=1)
    positions = jnp.arange(T_LOC)

    def owner_row(end_row):
        return jnp.searchsorted(end_row, positions, side='right')

    owner_seq = jax.vmap(owner_row)(count_ends)
    owner_seq = jax.random.permutation(perm_key, owner_seq, axis=1, independent=True)
    owner_safe = jnp.minimum(owner_seq, GROUP - 1)
    hot_match = hot_owner[None, :] == owners[:, None]
    has_hot = jnp.any(hot_match, axis=1).astype(jnp.int32)
    skip_local = jnp.sum(jnp.where(hot_match, hot_local[None, :], 0), axis=1) + (1 - has_hot) * N_LOC
    pick_local = jax.random.randint(cold_key, (GROUP, T_LOC), 0, N_LOC - has_hot[owner_safe])
    pick_local = pick_local + (pick_local >= skip_local[owner_safe]).astype(jnp.int32)
    cold_ids = owner_safe * N_LOC + pick_local
    hot_list = hot_owner * N_LOC + hot_local
    hot_tok = hot_list[jax.random.randint(pick_key, (GROUP, T_LOC), 0, HOT_K)]
    tok_ids = jnp.where(owner_seq == GROUP, hot_tok, cold_ids)
    return tok_ids.reshape(TOKENS).astype(jnp.int32)


def normal_weights(w_key, shape, std):
    return (jax.random.normal(w_key, shape, jnp.float32) * std).astype(jnp.bfloat16)


def adapter_set(set_key, adapter_count):
    set_keys = jax.random.split(set_key, 6)
    b_std = 0.5 / (LORA_SCALE * R ** 0.5)
    return [
        normal_weights(set_keys[0], (adapter_count, D, R), D ** -0.5),
        normal_weights(set_keys[1], (adapter_count, R, F), b_std),
        normal_weights(set_keys[2], (adapter_count, D, R), D ** -0.5),
        normal_weights(set_keys[3], (adapter_count, R, F), b_std),
        normal_weights(set_keys[4], (adapter_count, F, R), F ** -0.5),
        normal_weights(set_keys[5], (adapter_count, R, D), b_std),
    ]


def setup_inputs(seed: int = 0, part: int = 0) -> dict:
    root_key = jax.random.key(seed)
    base_keys = jax.random.split(jax.random.fold_in(root_key, 1), 3)
    route_key = jax.random.fold_in(root_key, 3)
    hot_owner, hot_local = draw_hot(jax.random.fold_in(route_key, 2))
    tok_ids = draw_ids(jax.random.fold_in(jax.random.fold_in(route_key, 1), part), hot_owner, hot_local)
    x_key = jax.random.fold_in(jax.random.fold_in(root_key, 5), part)
    store_set = adapter_set(jax.random.fold_in(root_key, 2), ADAPTERS)
    hot_set = adapter_set(jax.random.fold_in(root_key, 4), HOT_K)
    return {
        'x': jax.random.normal(x_key, (TOKENS, D), jnp.float32).astype(jnp.bfloat16),
        'adapter_id': tok_ids,
        'w_gate': normal_weights(base_keys[0], (D, F), D ** -0.5),
        'w_up': normal_weights(base_keys[1], (D, F), D ** -0.5),
        'w_down': normal_weights(base_keys[2], (F, D), F ** -0.5),
        'a_gate': store_set[0],
        'b_gate': store_set[1],
        'a_up': store_set[2],
        'b_up': store_set[3],
        'a_down': store_set[4],
        'b_down': store_set[5],
        'hot_ids': (hot_owner * N_LOC + hot_local).astype(jnp.int32),
        'hot_a_gate': hot_set[0],
        'hot_b_gate': hot_set[1],
        'hot_a_up': hot_set[2],
        'hot_b_up': hot_set[3],
        'hot_a_down': hot_set[4],
        'hot_b_down': hot_set[5],
    }


def lora_delta(tok_rows, a_rows, b_rows):
    low_rank = jnp.einsum('td,tdr->tr', tok_rows.astype(jnp.float32), a_rows.astype(jnp.float32)).astype(jnp.bfloat16)
    delta_f = jnp.einsum('tr,trf->tf', low_rank.astype(jnp.float32), b_rows.astype(jnp.float32))
    return (LORA_SCALE * delta_f).astype(jnp.bfloat16)


def reference(x, adapter_id, w_gate, w_up, w_down, a_gate, b_gate, a_up, b_up, a_down, b_down, hot_ids, hot_a_gate, hot_b_gate, hot_a_up, hot_b_up, hot_a_down, hot_b_down):
    def block_out(block_args):
        tok_rows, tok_ids = block_args
        hot_match = tok_ids[:, None] == hot_ids[None, :]
        is_hot = jnp.any(hot_match, axis=1)
        hot_slot = jnp.sum(jnp.where(hot_match, jnp.arange(HOT_K)[None, :], 0), axis=1)

        def chosen(store_set, hot_copy):
            return jnp.where(is_hot[:, None, None], hot_copy[hot_slot], store_set[tok_ids])

        gate_act = jnp.dot(tok_rows, w_gate, preferred_element_type=jnp.float32) + lora_delta(tok_rows, chosen(a_gate, hot_a_gate), chosen(b_gate, hot_b_gate)).astype(jnp.float32)
        up_act = jnp.dot(tok_rows, w_up, preferred_element_type=jnp.float32) + lora_delta(tok_rows, chosen(a_up, hot_a_up), chosen(b_up, hot_b_up)).astype(jnp.float32)
        hidden = (jax.nn.silu(gate_act) * up_act).astype(jnp.bfloat16)
        down_out = jnp.dot(hidden, w_down, preferred_element_type=jnp.float32) + lora_delta(hidden, chosen(a_down, hot_a_down), chosen(b_down, hot_b_down)).astype(jnp.float32)
        return (tok_rows.astype(jnp.float32) + down_out).astype(jnp.bfloat16)

    blocks = lax.map(block_out, (x.reshape(TOKENS // TOK_BLOCK, TOK_BLOCK, D), adapter_id.reshape(TOKENS // TOK_BLOCK, TOK_BLOCK)))
    return blocks.reshape(TOKENS, D)
```

```python
import functools

import jax
import jax.numpy as jnp
from jax import lax
from jax.experimental import pallas as pl
from jax.experimental.pallas import tpu as pltpu
from jax.sharding import PartitionSpec as P

LORA_ALPHA = 32
MESH = pl.DeviceIdType.MESH
BF = jnp.bfloat16
F32 = jnp.float32
NT = (((1,), (1,)), ((), ()))


def dot(a, b):
    return jnp.dot(a, b, preferred_element_type=F32)


def dot_nt(a, b):
    return lax.dot_general(a, b, NT, preferred_element_type=F32)


def peer_of(me, off):
    if off == 1:
        return me + 1 - 2 * (me % 2)
    if off == 2:
        return (me + 2) % 4
    return 3 - me


def route_kernel(n_local, cap, hot_ref, ids_ref, x_ref, xs_ref, sel_ref, back_ref, perm):
    toks = ids_ref.shape[1]
    blocks = 4
    spill = blocks * cap

    @pl.when(pl.program_id(0) == 0)
    def _():
        me = lax.axis_index("data")
        ids = ids_ref[...]
        owner = ids // n_local
        hot_slot = jnp.full_like(ids, -1)
        for j in range(hot_ref.shape[0]):
            hot_slot = jnp.where(ids == hot_ref[j], j, hot_slot)
        is_hot = hot_slot >= 0
        block = jnp.full_like(ids, 3)
        for off in (1, 2, 3):
            block = jnp.where(owner == peer_of(me, off), off - 1, block)
        cat = jnp.where(is_hot, blocks, block)
        onehot = (lax.broadcasted_iota(jnp.int32, (8, toks), 0) == cat).astype(F32)
        upper = (lax.broadcasted_iota(jnp.int32, (toks, toks), 0) < lax.broadcasted_iota(jnp.int32, (toks, toks), 1)).astype(BF)
        before = dot(onehot.astype(BF), upper)
        rank = jnp.sum(onehot * before, axis=0, keepdims=True).astype(jnp.int32)
        counts = jnp.sum(onehot, axis=1, keepdims=True).astype(jnp.int32)
        pos = jnp.where(is_hot, rank, cat * cap + rank)
        start = jnp.zeros((1, 1), jnp.int32)
        hot_pos = jnp.zeros_like(rank)
        for b in range(blocks):
            have = counts[b:b + 1, :]
            fill = cap - have
            hot_pos = jnp.where(rank >= start, b * cap + have + rank - start, hot_pos)
            start = start + fill
        hot_pos = jnp.where(rank >= start, spill + rank - start, hot_pos)
        pos = jnp.where(is_hot, hot_pos, pos)
        place = (lax.broadcasted_iota(jnp.int32, (toks, toks), 0) == pos).astype(F32)
        perm[...] = place.astype(BF)
        back_ref[...] = place.T.astype(BF)
        slot = jnp.where(is_hot, hot_slot, hot_ref.shape[0] + ids % n_local)
        pick = (lax.broadcasted_iota(jnp.int32, (128, toks), 0) == slot).astype(BF)
        sel_ref[...] = dot_nt(place.astype(BF), pick).astype(BF)

    xs_ref[...] = dot(perm[...], x_ref[...]).astype(BF)


def route(x, ids, hot_ids, n_local, cap):
    toks, width = x.shape
    chunk = 1024
    return pl.pallas_call(
        functools.partial(route_kernel, n_local, cap),
        grid=(width // chunk,),
        in_specs=[
            pl.BlockSpec(memory_space=pltpu.SMEM),
            pl.BlockSpec((1, toks), lambda i: (0, 0)),
            pl.BlockSpec((toks, chunk), lambda i: (0, i)),
        ],
        out_specs=[
            pl.BlockSpec((toks, chunk), lambda i: (0, i)),
            pl.BlockSpec((toks, 128), lambda i: (0, 0)),
            pl.BlockSpec((toks, toks), lambda i: (0, 0)),
        ],
        out_shape=[
            jax.ShapeDtypeStruct((toks, width), BF),
            jax.ShapeDtypeStruct((toks, 128), BF),
            jax.ShapeDtypeStruct((toks, toks), BF),
        ],
        scratch_shapes=[pltpu.VMEM((toks, toks), BF)],
    )(hot_ids, ids.reshape(1, toks), x)


def unroute_kernel(back_ref, ys_ref, out_ref):
    out_ref[...] = dot(back_ref[...], ys_ref[...]).astype(BF)


def unroute(back, ys):
    toks, width = ys.shape
    chunk = 1024
    return pl.pallas_call(
        unroute_kernel,
        grid=(width // chunk,),
        in_specs=[pl.BlockSpec((toks, toks), lambda i: (0, 0)), pl.BlockSpec((toks, chunk), lambda i: (0, i))],
        out_specs=pl.BlockSpec((toks, chunk), lambda i: (0, i)),
        out_shape=jax.ShapeDtypeStruct((toks, width), BF),
    )(back, ys)


FB = 256
SLOTS = 3
EARLY = 18


def mlp_kernel(scale, cap,
               xs, sel, wg, wu, wd, agh, agc, bgh, bgc, auh, auc, buh, buc, adh, adc, bdh, bdc,
               ys,
               xv, selv, hv, wbuf, lbuf, abuf, lowg, lowu, lowd, lowacc_h, lowacc_c, acc, ybuf,
               x_sem, xr_send, xr_recv, s_sem, sr_send, sr_recv, w_sem, l_sem, a_sem, y_send, y_recv, y_sem):
    me = lax.axis_index("data")
    toks, d = xs.shape
    f = wg.shape[1]
    half = toks // 2
    kh = agh.shape[0]
    kc = agc.shape[0]
    kk = kh + kc
    fblocks = f // FB
    dblocks = d // FB
    fh = f // 2
    n_gu = EARLY + (fblocks - EARLY) + EARLY
    n_steps = n_gu + 2 * dblocks

    barrier = pltpu.get_barrier_semaphore()
    for off in (1, 2, 3):
        pl.semaphore_signal(barrier, inc=1, device_id={"data": peer_of(me, off)}, device_id_type=MESH)

    def cols(i):
        return pl.ds(pl.multiple_of(i * FB, FB), FB)

    def gu_copies(blk, slot, cold):
        c = cols(blk)
        out = [
            pltpu.make_async_copy(wg.at[:, c], wbuf.at[slot, pl.ds(0, d)], w_sem.at[slot, 0]),
            pltpu.make_async_copy(wu.at[:, c], wbuf.at[slot, pl.ds(d, d)], w_sem.at[slot, 1]),
            pltpu.make_async_copy(bgh.at[:, c], lbuf.at[slot, 0, pl.ds(0, kh)], l_sem.at[slot, 0]),
            pltpu.make_async_copy(buh.at[:, c], lbuf.at[slot, 1, pl.ds(0, kh)], l_sem.at[slot, 1]),
            pltpu.make_async_copy(adh.at[:, c], lbuf.at[slot, 2, pl.ds(0, kh)], l_sem.at[slot, 2]),
        ]
        if cold:
            out += [
                pltpu.make_async_copy(bgc.at[:, c], lbuf.at[slot, 0, pl.ds(kh, kc)], l_sem.at[slot, 3]),
                pltpu.make_async_copy(buc.at[:, c], lbuf.at[slot, 1, pl.ds(kh, kc)], l_sem.at[slot, 4]),
                pltpu.make_async_copy(adc.at[:, c], lbuf.at[slot, 2, pl.ds(kh, kc)], l_sem.at[slot, 5]),
            ]
        return out

    def d_copies(blk, part, slot, low):
        c = cols(blk)
        rows = pl.ds(pl.multiple_of(part * fh, 256), fh)
        out = [pltpu.make_async_copy(wd.at[rows, c], wbuf.at[slot, pl.ds(0, fh)], w_sem.at[slot, 0])]
        if low:
            out += [
                pltpu.make_async_copy(bdh.at[:, c], lbuf.at[slot, 0, pl.ds(0, kh)], l_sem.at[slot, 0]),
                pltpu.make_async_copy(bdc.at[:, c], lbuf.at[slot, 0, pl.ds(kh, kc)], l_sem.at[slot, 3]),
            ]
        return out

    def issue(t):
        slot = t % SLOTS

        @pl.when(t < EARLY)
        def _():
            for c in gu_copies(t, slot, False):
                c.start()

        @pl.when((t >= EARLY) & (t < n_gu))
        def _():
            q = t - EARLY
            j = q // 3
            r = q % 3
            blk = jnp.where(r < 2, EARLY + 2 * j + r, j)
            for c in gu_copies(blk, slot, True):
                c.start()

        @pl.when((t >= n_gu) & (t < n_steps))
        def _():
            q = t - n_gu

            @pl.when(q % 2 == 0)
            def _():
                for c in d_copies(q // 2, 0, slot, False):
                    c.start()

            @pl.when(q % 2 == 1)
            def _():
                for c in d_copies(q // 2, 1, slot, True):
                    c.start()

    def a_copy(i, slot):
        if i < 2:
            src = (agh, auh)[i]
        else:
            c = i - 2
            src = (agc, auc)[c // 4].at[pl.ds((c % 4) * 256, 256)]
        return pltpu.make_async_copy(src, abuf.at[slot], a_sem.at[slot])

    near = pl.ds(half, half)
    far = pl.ds(0, half)
    own = pl.ds(3 * cap, cap)
    local_x = pltpu.make_async_copy(xs.at[near], xv.at[near], x_sem.at[0])
    local_s = pltpu.make_async_copy(sel.at[near], selv.at[near], s_sem.at[0])
    own_x = pltpu.make_async_copy(xs.at[own], xv.at[own], x_sem.at[1])
    own_s = pltpu.make_async_copy(sel.at[own], selv.at[own], s_sem.at[1])
    local_x.start()
    local_s.start()
    a_copy(0, 0).start()
    issue(0)
    a_copy(1, 1).start()
    own_x.start()
    own_s.start()
    a_copy(2, 2).start()
    issue(1)

    pl.semaphore_wait(barrier, 3)
    moves = []
    for off in (2, 3, 1):
        rows = pl.ds((off - 1) * cap, cap)
        for src, dst, snd, rcv in ((sel, selv, sr_send, sr_recv), (xs, xv, xr_send, xr_recv)):
            m = pltpu.make_async_remote_copy(
                src_ref=src.at[rows], dst_ref=dst.at[rows], send_sem=snd.at[off - 1], recv_sem=rcv.at[off - 1],
                device_id={"data": peer_of(me, off)}, device_id_type=MESH)
            m.start()
            moves.append(m)

    def mask(rows, first):
        row = lax.broadcasted_iota(jnp.int32, (128, 256), 0)
        col = lax.broadcasted_iota(jnp.int32, (128, 256), 1)
        spread = (row == first // 64 + col // 64).astype(BF)
        return dot(selv[rows, :], spread).astype(BF)

    def low_x(rows, slot, dst, first):
        low = dot_nt(xv[rows, :], abuf[slot]).astype(BF)
        dst[rows, first:first + 256] = low * mask(rows, first)

    lowacc_h[...] = jnp.zeros_like(lowacc_h)
    lowacc_c[...] = jnp.zeros_like(lowacc_c)
    local_x.wait()
    local_s.wait()
    a_copy(0, 0).wait()
    low_x(near, 0, lowg, 0)
    a_copy(1, 1).wait()
    low_x(near, 1, lowu, 0)

    def delta(low, b):
        return (scale * dot(low, b)).astype(BF).astype(F32)

    def hidden(rows, blk, slot, k):
        g = dot(xv[rows, :], wbuf[slot, 0:d]) + delta(lowg[rows, 0:k], lbuf[slot, 0, 0:k])
        u = dot(xv[rows, :], wbuf[slot, d:2 * d]) + delta(lowu[rows, 0:k], lbuf[slot, 1, 0:k])
        h = (jax.nn.silu(g) * u).astype(BF)
        hv[rows, cols(blk)] = h
        lowacc_h[rows, :] += dot_nt(h, lbuf[slot, 2, 0:kh])
        if k > kh:
            lowacc_c[rows, :] += dot_nt(h, lbuf[slot, 2, kh:kk])

    def early(t, carry):
        slot = t % SLOTS
        issue(t + 2)
        for c in gu_copies(t, slot, False):
            c.wait()
        hidden(near, t, slot, kh)
        return carry

    lax.fori_loop(0, EARLY, early, 0)

    own_x.wait()
    own_s.wait()
    for m in moves:
        m.wait()
    for i in range(10):
        slot = i % 3
        if i >= 2:
            a_copy(i, slot).wait()
        dst = lowg if i == 0 or 2 <= i < 6 else lowu
        first = 0 if i < 2 else 256 * (1 + (i - 2) % 4)
        low_x(far, slot, dst, first)
        if i + 3 < 10:
            a_copy(i + 3, slot).start()

    def group(j, carry):
        def both(r, carry):
            t = EARLY + 3 * j + r
            slot = t % SLOTS
            blk = EARLY + 2 * j + r
            issue(t + 2)
            for c in gu_copies(blk, slot, True):
                c.wait()
            hidden(near, blk, slot, kh)
            hidden(far, blk, slot, kk)
            return carry

        lax.fori_loop(0, 2, both, 0)
        t = EARLY + 3 * j + 2
        slot = t % SLOTS
        issue(t + 2)
        for c in gu_copies(j, slot, True):
            c.wait()
        hidden(far, j, slot, kk)
        return carry

    lax.fori_loop(0, EARLY, group, 0)

    for i in range(kk // 256):
        part = slice(256 * i, 256 * (i + 1))
        if i == 0:
            lowd[near, part] = lowacc_h[near, :].astype(BF) * mask(near, 0)
            lowd[far, part] = lowacc_h[far, :].astype(BF) * mask(far, 0)
        else:
            lowd[far, part] = lowacc_c[:, 256 * (i - 1):256 * i].astype(BF) * mask(far, 256 * i)

    def back_copies(blk):
        p = blk % 2
        c = cols(blk)
        out = []
        for off in (2, 3, 1):
            rows = pl.ds((off - 1) * cap, cap)
            out.append(pltpu.make_async_remote_copy(
                src_ref=ybuf.at[p, rows], dst_ref=ys.at[rows, c], send_sem=y_send.at[p, off - 1],
                recv_sem=y_recv.at[off - 1], device_id={"data": peer_of(me, off)}, device_id_type=MESH))
        mine = pl.ds(3 * cap, toks - 3 * cap)
        return out, pltpu.make_async_copy(ybuf.at[p, mine], ys.at[mine, c], y_sem.at[p])

    def send_back(blk):
        remote, local = back_copies(blk)
        for m in remote:
            m.start()
        local.start()

    def sent(blk):
        remote, local = back_copies(blk)
        for m in remote:
            m.wait_send()
        local.wait()

    def down(i, carry):
        t = n_gu + 2 * i
        slot = t % SLOTS
        issue(t + 2)
        for c in d_copies(i, 0, slot, False):
            c.wait()
        acc[...] = dot(hv[:, 0:fh], wbuf[slot, 0:fh])

        @pl.when(i > 0)
        def _():
            send_back(i - 1)

        t = t + 1
        slot = t % SLOTS
        issue(t + 2)
        for c in d_copies(i, 1, slot, True):
            c.wait()

        @pl.when(i > 1)
        def _():
            sent(i - 2)

        y = acc[...] + dot(hv[:, fh:f], wbuf[slot, 0:fh])
        acc[...] = y
        p = i % 2
        for rows, k in ((near, kh), (far, kk)):
            out = acc[rows, :] + delta(lowd[rows, 0:k], lbuf[slot, 0, 0:k])
            ybuf[p, rows, :] = (xv[rows, cols(i)].astype(F32) + out).astype(BF)
        return carry

    lax.fori_loop(0, dblocks, down, 0)
    send_back(dblocks - 1)
    sent(dblocks - 2)
    sent(dblocks - 1)
    for off in (2, 3, 1):
        rows = pl.ds((off - 1) * cap, cap)
        pltpu.make_async_remote_copy(
            src_ref=ys.at[rows], dst_ref=ys.at[rows], send_sem=y_send.at[0, off - 1], recv_sem=y_recv.at[off - 1],
            device_id={"data": peer_of(me, off)}, device_id_type=MESH).wait_recv()


def mlp(scale, cap, xs, sel, ws, cold, hot):
    toks, d = xs.shape
    f = ws[0].shape[1]
    kh, kc = hot[0].shape[0], cold[0].shape[0]
    kk = kh + kc
    half = toks // 2
    pairs = [m for h, c in zip(hot, cold) for m in (h, c)]
    dma = pltpu.SemaphoreType.DMA
    return pl.pallas_call(
        functools.partial(mlp_kernel, scale, cap),
        in_specs=[pl.BlockSpec(memory_space=pl.ANY)] * 17,
        out_specs=pl.BlockSpec(memory_space=pl.ANY),
        out_shape=jax.ShapeDtypeStruct((toks, d), BF),
        scratch_shapes=[
            pltpu.VMEM((toks, d), BF),
            pltpu.VMEM((toks, 128), BF),
            pltpu.VMEM((toks, f), BF),
            pltpu.VMEM((SLOTS, 2 * d, FB), BF),
            pltpu.VMEM((SLOTS, 3, kk, FB), BF),
            pltpu.VMEM((3, 256, d), BF),
            pltpu.VMEM((toks, kk), BF),
            pltpu.VMEM((toks, kk), BF),
            pltpu.VMEM((toks, kk), BF),
            pltpu.VMEM((toks, kh), F32),
            pltpu.VMEM((half, kc), F32),
            pltpu.VMEM((toks, FB), F32),
            pltpu.VMEM((2, toks, FB), BF),
            dma((2,)), dma((3,)), dma((3,)), dma((2,)), dma((3,)), dma((3,)),
            dma((SLOTS, 2)), dma((SLOTS, 6)), dma((3,)), dma((2, 3)), dma((3,)), dma((2,)),
        ],
        compiler_params=pltpu.CompilerParams(
            collective_id=0, has_side_effects=True, vmem_limit_bytes=63 * 1024 * 1024),
    )(xs, sel, *ws, *pairs)


def solution(mesh):
    group = mesh.shape["data"]
    token_spec = P(("replica", "data"), None)
    store_spec = P("data", None, None)
    full_mat = P(None, None)
    full_set = P(None, None, None)
    in_specs = (token_spec, P(("replica", "data")), full_mat, full_mat, full_mat) + (store_spec,) * 6 + (P(None),) + (full_set,) * 6

    def device_step(x, adapter_id, w_gate, w_up, w_down, a_gate, b_gate, a_up, b_up, a_down, b_down, hot_ids, hot_a_gate, hot_b_gate, hot_a_up, hot_b_up, hot_a_down, hot_b_down):
        cap = x.shape[0] // (2 * group)
        scale = LORA_ALPHA / a_gate.shape[2]

        def flat_a(a):
            return jnp.swapaxes(a, 1, 2).reshape(-1, a.shape[1])

        def flat_b(b):
            return b.reshape(-1, b.shape[2])

        xs, sel, back = route(x, adapter_id, hot_ids, a_gate.shape[0], cap)
        cold = [flat_a(a_gate), flat_b(b_gate), flat_a(a_up), flat_b(b_up), flat_a(a_down), flat_b(b_down)]
        hot = [flat_a(hot_a_gate), flat_b(hot_b_gate), flat_a(hot_a_up), flat_b(hot_b_up), flat_a(hot_a_down), flat_b(hot_b_down)]
        ys = mlp(scale, cap, xs, sel, (w_gate, w_up, w_down), cold, hot)
        return unroute(back, ys)

    return jax.shard_map(device_step, mesh=mesh, in_specs=in_specs, out_specs=token_spec, check_vma=False)
```

```python
import functools

import jax
import jax.numpy as jnp
from jax import lax
from jax.experimental import pallas as pl
from jax.experimental.pallas import tpu as pltpu
from jax.sharding import PartitionSpec as P

LORA_ALPHA = 32
MESH = pl.DeviceIdType.MESH
BF = jnp.bfloat16
F32 = jnp.float32
NT = (((1,), (1,)), ((), ()))


def dot(a, b):
    return jnp.dot(a, b, preferred_element_type=F32)


def dot_nt(a, b):
    return lax.dot_general(a, b, NT, preferred_element_type=F32)


def peer_of(me, off):
    if off == 1:
        return me + 1 - 2 * (me % 2)
    if off == 2:
        return (me + 2) % 4
    return 3 - me


def route_kernel(n_local, cap, hot_ref, ids_ref, x_ref, xs_ref, sel_ref, back_ref, perm):
    toks = ids_ref.shape[1]
    blocks = 4
    spill = blocks * cap

    @pl.when(pl.program_id(0) == 0)
    def _():
        me = lax.axis_index("data")
        ids = ids_ref[...]
        owner = ids // n_local
        hot_slot = jnp.full_like(ids, -1)
        for j in range(hot_ref.shape[0]):
            hot_slot = jnp.where(ids == hot_ref[j], j, hot_slot)
        is_hot = hot_slot >= 0
        block = jnp.full_like(ids, 3)
        for off in (1, 2, 3):
            block = jnp.where(owner == peer_of(me, off), off - 1, block)
        cat = jnp.where(is_hot, blocks, block)
        onehot = (lax.broadcasted_iota(jnp.int32, (8, toks), 0) == cat).astype(F32)
        upper = (lax.broadcasted_iota(jnp.int32, (toks, toks), 0) < lax.broadcasted_iota(jnp.int32, (toks, toks), 1)).astype(BF)
        before = dot(onehot.astype(BF), upper)
        rank = jnp.sum(onehot * before, axis=0, keepdims=True).astype(jnp.int32)
        counts = jnp.sum(onehot, axis=1, keepdims=True).astype(jnp.int32)
        pos = jnp.where(is_hot, rank, cat * cap + rank)
        start = jnp.zeros((1, 1), jnp.int32)
        hot_pos = jnp.zeros_like(rank)
        for b in range(blocks):
            have = counts[b:b + 1, :]
            fill = cap - have
            hot_pos = jnp.where(rank >= start, b * cap + have + rank - start, hot_pos)
            start = start + fill
        hot_pos = jnp.where(rank >= start, spill + rank - start, hot_pos)
        pos = jnp.where(is_hot, hot_pos, pos)
        place = (lax.broadcasted_iota(jnp.int32, (toks, toks), 0) == pos).astype(F32)
        perm[...] = place.astype(BF)
        back_ref[...] = place.T.astype(BF)
        slot = jnp.where(is_hot, hot_slot, hot_ref.shape[0] + ids % n_local)
        pick = (lax.broadcasted_iota(jnp.int32, (128, toks), 0) == slot).astype(BF)
        sel_ref[...] = dot_nt(place.astype(BF), pick).astype(BF)

    xs_ref[...] = dot(perm[...], x_ref[...]).astype(BF)


def route(x, ids, hot_ids, n_local, cap):
    toks, width = x.shape
    chunk = 1024
    return pl.pallas_call(
        functools.partial(route_kernel, n_local, cap),
        grid=(width // chunk,),
        in_specs=[
            pl.BlockSpec(memory_space=pltpu.SMEM),
            pl.BlockSpec((1, toks), lambda i: (0, 0)),
            pl.BlockSpec((toks, chunk), lambda i: (0, i)),
        ],
        out_specs=[
            pl.BlockSpec((toks, chunk), lambda i: (0, i)),
            pl.BlockSpec((toks, 128), lambda i: (0, 0)),
            pl.BlockSpec((toks, toks), lambda i: (0, 0)),
        ],
        out_shape=[
            jax.ShapeDtypeStruct((toks, width), BF),
            jax.ShapeDtypeStruct((toks, 128), BF),
            jax.ShapeDtypeStruct((toks, toks), BF),
        ],
        scratch_shapes=[pltpu.VMEM((toks, toks), BF)],
    )(hot_ids, ids.reshape(1, toks), x)


def unroute_kernel(back_ref, ys_ref, out_ref):
    out_ref[...] = dot(back_ref[...], ys_ref[...]).astype(BF)


def unroute(back, ys):
    toks, width = ys.shape
    chunk = 1024
    return pl.pallas_call(
        unroute_kernel,
        grid=(width // chunk,),
        in_specs=[pl.BlockSpec((toks, toks), lambda i: (0, 0)), pl.BlockSpec((toks, chunk), lambda i: (0, i))],
        out_specs=pl.BlockSpec((toks, chunk), lambda i: (0, i)),
        out_shape=jax.ShapeDtypeStruct((toks, width), BF),
    )(back, ys)


FB = 256
SLOTS = 3
EARLY = 18
AD_STEPS = 6


def mlp_kernel(scale, cap,
               xs, sel, wg, wu, wd, agh, agc, bgh, bgc, auh, auc, buh, buc, adh, adc, bdh, bdc,
               ys,
               xv, selv, hv, wbuf, lbuf, abuf, lowg, lowu, lowacc_h, lowacc_c, ybuf,
               x_sem, xr_send, xr_recv, s_sem, sr_send, sr_recv, w_sem, l_sem, d_sem, a_sem, y_send, y_recv, y_sem):
    me = lax.axis_index("data")
    toks, d = xs.shape
    f = wg.shape[1]
    half = toks // 2
    kh = agh.shape[0]
    kc = agc.shape[0]
    kk = kh + kc
    fblocks = f // FB
    dblocks = d // FB
    per = fblocks // AD_STEPS
    n_gu = EARLY + (fblocks - EARLY) + EARLY
    n_ad = n_gu + AD_STEPS
    n_steps = n_ad + dblocks

    barrier = pltpu.get_barrier_semaphore()
    for off in (1, 2, 3):
        pl.semaphore_signal(barrier, inc=1, device_id={"data": peer_of(me, off)}, device_id_type=MESH)

    def cols(i):
        return pl.ds(pl.multiple_of(i * FB, FB), FB)

    def gu_copies(blk, slot, cold):
        c = cols(blk)
        out = [
            pltpu.make_async_copy(wg.at[:, c], wbuf.at[slot, pl.ds(0, d)], w_sem.at[slot, 0]),
            pltpu.make_async_copy(wu.at[:, c], wbuf.at[slot, pl.ds(d, d)], w_sem.at[slot, 1]),
            pltpu.make_async_copy(bgh.at[:, c], lbuf.at[slot, 0, pl.ds(0, kh)], l_sem.at[slot, 0]),
            pltpu.make_async_copy(buh.at[:, c], lbuf.at[slot, 1, pl.ds(0, kh)], l_sem.at[slot, 1]),
        ]
        if cold:
            out += [
                pltpu.make_async_copy(bgc.at[:, c], lbuf.at[slot, 0, pl.ds(kh, kc)], l_sem.at[slot, 2]),
                pltpu.make_async_copy(buc.at[:, c], lbuf.at[slot, 1, pl.ds(kh, kc)], l_sem.at[slot, 3]),
            ]
        return out

    def ad_copies(blk, slot):
        out = []
        for q in range(per):
            c = cols(blk * per + q)
            out.append(pltpu.make_async_copy(adh.at[:, c], wbuf.at[slot, pl.ds(q * kk, kh)], d_sem.at[slot, 2 * q]))
            out.append(pltpu.make_async_copy(adc.at[:, c], wbuf.at[slot, pl.ds(q * kk + kh, kc)], d_sem.at[slot, 2 * q + 1]))
        return out

    def d_copies(blk, slot):
        c = cols(blk)
        return [
            pltpu.make_async_copy(wd.at[:, c], wbuf.at[slot], w_sem.at[slot, 0]),
            pltpu.make_async_copy(bdh.at[:, c], lbuf.at[slot, 0, pl.ds(0, kh)], l_sem.at[slot, 0]),
            pltpu.make_async_copy(bdc.at[:, c], lbuf.at[slot, 0, pl.ds(kh, kc)], l_sem.at[slot, 2]),
        ]

    def issue(t):
        slot = t % SLOTS

        @pl.when(t < EARLY)
        def _():
            for c in gu_copies(t, slot, False):
                c.start()

        @pl.when((t >= EARLY) & (t < n_gu))
        def _():
            q = t - EARLY
            j = q // 3
            r = q % 3
            blk = jnp.where(r < 2, EARLY + 2 * j + r, j)
            for c in gu_copies(blk, slot, True):
                c.start()

        @pl.when((t >= n_gu) & (t < n_ad))
        def _():
            for c in ad_copies(t - n_gu, slot):
                c.start()

        @pl.when((t >= n_ad) & (t < n_steps))
        def _():
            for c in d_copies(t - n_ad, slot):
                c.start()

    def a_copy(i, slot):
        if i < 2:
            src = (agh, auh)[i]
        else:
            c = i - 2
            src = (agc, auc)[c // 4].at[pl.ds((c % 4) * 256, 256)]
        return pltpu.make_async_copy(src, abuf.at[slot], a_sem.at[slot])

    near = pl.ds(half, half)
    far = pl.ds(0, half)
    own = pl.ds(3 * cap, cap)
    local_x = pltpu.make_async_copy(xs.at[near], xv.at[near], x_sem.at[0])
    local_s = pltpu.make_async_copy(sel.at[near], selv.at[near], s_sem.at[0])
    own_x = pltpu.make_async_copy(xs.at[own], xv.at[own], x_sem.at[1])
    own_s = pltpu.make_async_copy(sel.at[own], selv.at[own], s_sem.at[1])
    local_x.start()
    local_s.start()
    a_copy(0, 0).start()
    issue(0)
    a_copy(1, 1).start()
    own_x.start()
    own_s.start()
    a_copy(2, 2).start()
    issue(1)

    pl.semaphore_wait(barrier, 3)
    moves = []
    for off in (2, 3, 1):
        rows = pl.ds((off - 1) * cap, cap)
        for src, dst, snd, rcv in ((sel, selv, sr_send, sr_recv), (xs, xv, xr_send, xr_recv)):
            m = pltpu.make_async_remote_copy(
                src_ref=src.at[rows], dst_ref=dst.at[rows], send_sem=snd.at[off - 1], recv_sem=rcv.at[off - 1],
                device_id={"data": peer_of(me, off)}, device_id_type=MESH)
            m.start()
            moves.append(m)

    def mask(rows, first):
        row = lax.broadcasted_iota(jnp.int32, (128, 256), 0)
        col = lax.broadcasted_iota(jnp.int32, (128, 256), 1)
        spread = (row == first // 64 + col // 64).astype(BF)
        return dot(selv[rows, :], spread).astype(BF)

    def low_x(rows, slot, dst, first):
        low = dot_nt(xv[rows, :], abuf[slot]).astype(BF)
        dst[rows, first:first + 256] = low * mask(rows, first)

    lowacc_h[...] = jnp.zeros_like(lowacc_h)
    lowacc_c[...] = jnp.zeros_like(lowacc_c)
    local_x.wait()
    local_s.wait()
    a_copy(0, 0).wait()
    low_x(near, 0, lowg, 0)
    a_copy(1, 1).wait()
    low_x(near, 1, lowu, 0)

    def delta(low, b):
        return (scale * dot(low, b)).astype(BF).astype(F32)

    def hidden(rows, blk, slot, k):
        g = dot(xv[rows, :], wbuf[slot, 0:d]) + delta(lowg[rows, 0:k], lbuf[slot, 0, 0:k])
        u = dot(xv[rows, :], wbuf[slot, d:2 * d]) + delta(lowu[rows, 0:k], lbuf[slot, 1, 0:k])
        hv[rows, cols(blk)] = (jax.nn.silu(g) * u).astype(BF)

    def early(t, carry):
        slot = t % SLOTS
        issue(t + 2)
        for c in gu_copies(t, slot, False):
            c.wait()
        hidden(near, t, slot, kh)
        return carry

    lax.fori_loop(0, EARLY, early, 0)

    own_x.wait()
    own_s.wait()
    for m in moves:
        m.wait()
    for i in range(10):
        slot = i % 3
        if i >= 2:
            a_copy(i, slot).wait()
        dst = lowg if i == 0 or 2 <= i < 6 else lowu
        first = 0 if i < 2 else 256 * (1 + (i - 2) % 4)
        low_x(far, slot, dst, first)
        if i + 3 < 10:
            a_copy(i + 3, slot).start()

    def group(j, carry):
        def both(r, carry):
            t = EARLY + 3 * j + r
            slot = t % SLOTS
            blk = EARLY + 2 * j + r
            issue(t + 2)
            for c in gu_copies(blk, slot, True):
                c.wait()
            hidden(near, blk, slot, kh)
            hidden(far, blk, slot, kk)
            return carry

        lax.fori_loop(0, 2, both, 0)
        t = EARLY + 3 * j + 2
        slot = t % SLOTS
        issue(t + 2)
        for c in gu_copies(j, slot, True):
            c.wait()
        hidden(far, j, slot, kk)
        return carry

    lax.fori_loop(0, EARLY, group, 0)

    def low_h(i, carry):
        t = n_gu + i
        slot = t % SLOTS
        issue(t + 2)
        for c in ad_copies(i, slot):
            c.wait()
        first = i * per
        hot_sum, cold_sum = lowacc_h[...], lowacc_c[...]
        for q in range(per):
            c = cols(first + q)
            hot_sum += dot_nt(hv[:, c], wbuf[slot, q * kk:q * kk + kh])
            cold_sum += dot_nt(hv[far, c], wbuf[slot, q * kk + kh:(q + 1) * kk])
        lowacc_h[...] = hot_sum
        lowacc_c[...] = cold_sum
        return carry

    lax.fori_loop(0, AD_STEPS, low_h, 0)

    lowd = lowg
    for i in range(kk // 256):
        part = slice(256 * i, 256 * (i + 1))
        if i == 0:
            lowd[near, part] = lowacc_h[near, :].astype(BF) * mask(near, 0)
            lowd[far, part] = lowacc_h[far, :].astype(BF) * mask(far, 0)
        else:
            lowd[far, part] = lowacc_c[:, 256 * (i - 1):256 * i].astype(BF) * mask(far, 256 * i)

    def back_copies(blk):
        p = blk % 2
        c = cols(blk)
        out = []
        for off in (2, 3, 1):
            rows = pl.ds((off - 1) * cap, cap)
            out.append(pltpu.make_async_remote_copy(
                src_ref=ybuf.at[p, rows], dst_ref=ys.at[rows, c], send_sem=y_send.at[p, off - 1],
                recv_sem=y_recv.at[off - 1], device_id={"data": peer_of(me, off)}, device_id_type=MESH))
        mine = pl.ds(3 * cap, toks - 3 * cap)
        return out, pltpu.make_async_copy(ybuf.at[p, mine], ys.at[mine, c], y_sem.at[p])

    def send_back(blk):
        remote, local = back_copies(blk)
        for m in remote:
            m.start()
        local.start()

    def sent(blk):
        remote, local = back_copies(blk)
        for m in remote:
            m.wait_send()
        local.wait()

    def down(i, carry):
        t = n_ad + i
        slot = t % SLOTS

        @pl.when(i > 0)
        def _():
            send_back(i - 1)

        @pl.when(i > 1)
        def _():
            sent(i - 2)

        issue(t + 2)
        for c in d_copies(i, slot):
            c.wait()
        p = i % 2
        for rows, k in ((near, kh), (far, kk)):
            y = dot(hv[rows, :], wbuf[slot]) + delta(lowd[rows, 0:k], lbuf[slot, 0, 0:k])
            ybuf[p, rows, :] = (xv[rows, cols(i)].astype(F32) + y).astype(BF)
        return carry

    lax.fori_loop(0, dblocks, down, 0)
    send_back(dblocks - 1)
    sent(dblocks - 2)
    sent(dblocks - 1)
    for off in (2, 3, 1):
        rows = pl.ds((off - 1) * cap, cap)
        pltpu.make_async_remote_copy(
            src_ref=ys.at[rows], dst_ref=ys.at[rows], send_sem=y_send.at[0, off - 1], recv_sem=y_recv.at[off - 1],
            device_id={"data": peer_of(me, off)}, device_id_type=MESH).wait_recv()


def mlp(scale, cap, xs, sel, ws, cold, hot):
    toks, d = xs.shape
    f = ws[0].shape[1]
    kh, kc = hot[0].shape[0], cold[0].shape[0]
    kk = kh + kc
    half = toks // 2
    pairs = [m for h, c in zip(hot, cold) for m in (h, c)]
    dma = pltpu.SemaphoreType.DMA
    return pl.pallas_call(
        functools.partial(mlp_kernel, scale, cap),
        in_specs=[pl.BlockSpec(memory_space=pl.ANY)] * 17,
        out_specs=pl.BlockSpec(memory_space=pl.ANY),
        out_shape=jax.ShapeDtypeStruct((toks, d), BF),
        scratch_shapes=[
            pltpu.VMEM((toks, d), BF),
            pltpu.VMEM((toks, 128), BF),
            pltpu.VMEM((toks, f), BF),
            pltpu.VMEM((SLOTS, f, FB), BF),
            pltpu.VMEM((SLOTS, 2, kk, FB), BF),
            pltpu.VMEM((3, 256, d), BF),
            pltpu.VMEM((toks, kk), BF),
            pltpu.VMEM((toks, kk), BF),
            pltpu.VMEM((toks, kh), F32),
            pltpu.VMEM((half, kc), F32),
            pltpu.VMEM((2, toks, FB), BF),
            dma((2,)), dma((3,)), dma((3,)), dma((2,)), dma((3,)), dma((3,)),
            dma((SLOTS, 2)), dma((SLOTS, 4)), dma((SLOTS, 2 * (f // FB // AD_STEPS))), dma((3,)), dma((2, 3)), dma((3,)), dma((2,)),
        ],
        compiler_params=pltpu.CompilerParams(
            collective_id=0, has_side_effects=True, vmem_limit_bytes=63 * 1024 * 1024),
    )(xs, sel, *ws, *pairs)


def solution(mesh):
    group = mesh.shape["data"]
    token_spec = P(("replica", "data"), None)
    store_spec = P("data", None, None)
    full_mat = P(None, None)
    full_set = P(None, None, None)
    in_specs = (token_spec, P(("replica", "data")), full_mat, full_mat, full_mat) + (store_spec,) * 6 + (P(None),) + (full_set,) * 6

    def device_step(x, adapter_id, w_gate, w_up, w_down, a_gate, b_gate, a_up, b_up, a_down, b_down, hot_ids, hot_a_gate, hot_b_gate, hot_a_up, hot_b_up, hot_a_down, hot_b_down):
        cap = x.shape[0] // (2 * group)
        scale = LORA_ALPHA / a_gate.shape[2]

        def flat_a(a):
            return jnp.swapaxes(a, 1, 2).reshape(-1, a.shape[1])

        def flat_b(b):
            return b.reshape(-1, b.shape[2])

        xs, sel, back = route(x, adapter_id, hot_ids, a_gate.shape[0], cap)
        cold = [flat_a(a_gate), flat_b(b_gate), flat_a(a_up), flat_b(b_up), flat_a(a_down), flat_b(b_down)]
        hot = [flat_a(hot_a_gate), flat_b(hot_b_gate), flat_a(hot_a_up), flat_b(hot_b_up), flat_a(hot_a_down), flat_b(hot_b_down)]
        ys = mlp(scale, cap, xs, sel, (w_gate, w_up, w_down), cold, hot)
        return unroute(back, ys)

    return jax.shard_map(device_step, mesh=mesh, in_specs=in_specs, out_specs=token_spec, check_vma=False)
```

```python
import functools

import jax
import jax.numpy as jnp
from jax import lax
from jax.experimental import pallas as pl
from jax.experimental.pallas import tpu as pltpu
from jax.sharding import PartitionSpec as P

LORA_ALPHA = 32
MESH = pl.DeviceIdType.MESH
BF = jnp.bfloat16
F32 = jnp.float32
NT = (((1,), (1,)), ((), ()))


def dot(a, b):
    return jnp.dot(a, b, preferred_element_type=F32)


def dot_nt(a, b):
    return lax.dot_general(a, b, NT, preferred_element_type=F32)


def peer_of(me, off):
    if off == 1:
        return me + 1 - 2 * (me % 2)
    if off == 2:
        return (me + 2) % 4
    return 3 - me


def placement(me, n_local, cap, hot_ref, ids):
    toks = ids.shape[1]
    blocks = 4
    owner = ids // n_local
    hot_slot = jnp.full_like(ids, -1)
    for j in range(hot_ref.shape[0]):
        hot_slot = jnp.where(ids == hot_ref[j], j, hot_slot)
    is_hot = hot_slot >= 0
    block = jnp.full_like(ids, 3)
    for off in (1, 2, 3):
        block = jnp.where(owner == peer_of(me, off), off - 1, block)
    cat = jnp.where(is_hot, blocks, block)
    onehot = (lax.broadcasted_iota(jnp.int32, (8, toks), 0) == cat).astype(F32)
    upper = (lax.broadcasted_iota(jnp.int32, (toks, toks), 0) < lax.broadcasted_iota(jnp.int32, (toks, toks), 1)).astype(BF)
    before = dot(onehot.astype(BF), upper)
    rank = jnp.sum(onehot * before, axis=0, keepdims=True).astype(jnp.int32)
    counts = jnp.sum(onehot, axis=1, keepdims=True).astype(jnp.int32)
    start = jnp.zeros((1, 1), jnp.int32)
    hot_pos = jnp.zeros_like(rank)
    for b in range(blocks):
        have = counts[b:b + 1, :]
        hot_pos = jnp.where(rank >= start, b * cap + have + rank - start, hot_pos)
        start = start + cap - have
    hot_pos = jnp.where(rank >= start, blocks * cap + rank - start, hot_pos)
    pos = jnp.where(is_hot, hot_pos, cat * cap + rank)
    place = (lax.broadcasted_iota(jnp.int32, (toks, toks), 0) == pos).astype(F32)
    slot = jnp.where(is_hot, hot_slot, hot_ref.shape[0] + ids % n_local)
    pick = (lax.broadcasted_iota(jnp.int32, (128, toks), 0) == slot).astype(BF)
    return place, pick


def unroute_kernel(back_ref, ys_ref, out_ref):
    out_ref[...] = dot(back_ref[...], ys_ref[...]).astype(BF)


def unroute(back, ys):
    toks, width = ys.shape
    chunk = 1280
    return pl.pallas_call(
        unroute_kernel,
        grid=(width // chunk,),
        in_specs=[pl.BlockSpec((toks, toks), lambda i: (0, 0)), pl.BlockSpec((toks, chunk), lambda i: (0, i))],
        out_specs=pl.BlockSpec((toks, chunk), lambda i: (0, i)),
        out_shape=jax.ShapeDtypeStruct((toks, width), BF),
    )(back, ys)


FB = 256
SLOTS = 3
EARLY = 18
AD_STEPS = 6


def mlp_kernel(scale, cap, n_local,
               hot_ids, ids, x, wg, wu, wd, agh, agc, bgh, bgc, auh, auc, buh, buc, adh, adc, bdh, bdc,
               ys, back,
               xv, selv, sels, perm, backv, hv, wbuf, lbuf, abuf, lowg, lowu, lowacc_h, lowacc_c, ybuf,
               x_sem, b_sem, xr_send, xr_recv, sr_send, sr_recv, w_sem, l_sem, d_sem, a_sem, y_send, y_recv, y_sem):
    me = lax.axis_index("data")
    toks, d = x.shape
    f = wg.shape[1]
    half = toks // 2
    kh = agh.shape[0]
    kc = agc.shape[0]
    kk = kh + kc
    fblocks = f // FB
    dblocks = d // FB
    per = fblocks // AD_STEPS
    n_gu = EARLY + (fblocks - EARLY) + EARLY
    n_ad = n_gu + AD_STEPS
    n_steps = n_ad + dblocks

    barrier = pltpu.get_barrier_semaphore()
    for off in (1, 2, 3):
        pl.semaphore_signal(barrier, inc=1, device_id={"data": peer_of(me, off)}, device_id_type=MESH)

    def cols(i):
        return pl.ds(pl.multiple_of(i * FB, FB), FB)

    def gu_copies(blk, slot, cold):
        c = cols(blk)
        out = [
            pltpu.make_async_copy(wg.at[:, c], wbuf.at[slot, pl.ds(0, d)], w_sem.at[slot, 0]),
            pltpu.make_async_copy(wu.at[:, c], wbuf.at[slot, pl.ds(d, d)], w_sem.at[slot, 1]),
            pltpu.make_async_copy(bgh.at[:, c], lbuf.at[slot, 0, pl.ds(0, kh)], l_sem.at[slot, 0]),
            pltpu.make_async_copy(buh.at[:, c], lbuf.at[slot, 1, pl.ds(0, kh)], l_sem.at[slot, 1]),
        ]
        if cold:
            out += [
                pltpu.make_async_copy(bgc.at[:, c], lbuf.at[slot, 0, pl.ds(kh, kc)], l_sem.at[slot, 2]),
                pltpu.make_async_copy(buc.at[:, c], lbuf.at[slot, 1, pl.ds(kh, kc)], l_sem.at[slot, 3]),
            ]
        return out

    def ad_copies(blk, slot):
        out = []
        for q in range(per):
            c = cols(blk * per + q)
            out.append(pltpu.make_async_copy(adh.at[:, c], wbuf.at[slot, pl.ds(q * kk, kh)], d_sem.at[slot, 2 * q]))
            out.append(pltpu.make_async_copy(adc.at[:, c], wbuf.at[slot, pl.ds(q * kk + kh, kc)], d_sem.at[slot, 2 * q + 1]))
        return out

    def d_copies(blk, slot):
        c = cols(blk)
        return [
            pltpu.make_async_copy(wd.at[:, c], wbuf.at[slot], w_sem.at[slot, 0]),
            pltpu.make_async_copy(bdh.at[:, c], lbuf.at[slot, 0, pl.ds(0, kh)], l_sem.at[slot, 0]),
            pltpu.make_async_copy(bdc.at[:, c], lbuf.at[slot, 0, pl.ds(kh, kc)], l_sem.at[slot, 2]),
        ]

    def issue(t):
        slot = t % SLOTS

        @pl.when(t < EARLY)
        def _():
            for c in gu_copies(t, slot, False):
                c.start()

        @pl.when((t >= EARLY) & (t < n_gu))
        def _():
            q = t - EARLY
            j = q // 3
            r = q % 3
            blk = jnp.where(r < 2, EARLY + 2 * j + r, j)
            for c in gu_copies(blk, slot, True):
                c.start()

        @pl.when((t >= n_gu) & (t < n_ad))
        def _():
            for c in ad_copies(t - n_gu, slot):
                c.start()

        @pl.when((t >= n_ad) & (t < n_steps))
        def _():
            for c in d_copies(t - n_ad, slot):
                c.start()

    def a_copy(i, slot):
        if i < 2:
            src = (agh, auh)[i]
        else:
            c = i - 2
            src = (agc, auc)[c // 4].at[pl.ds((c % 4) * 256, 256)]
        return pltpu.make_async_copy(src, abuf.at[slot], a_sem.at[slot])

    near = pl.ds(half, half)
    far = pl.ds(0, half)
    own = pl.ds(3 * cap, cap)
    chunk = 1024
    loads = [pltpu.make_async_copy(x.at[:, pl.ds(c, chunk)], hv.at[:, pl.ds(d + c, chunk)], x_sem.at[c // chunk])
             for c in range(0, d, chunk)]
    for c in loads:
        c.start()
    a_copy(0, 0).start()
    a_copy(1, 1).start()
    issue(0)
    place, pick = placement(me, n_local, cap, hot_ids, ids[...])
    perm[...] = place.astype(BF)
    for c, load in zip(range(0, d, chunk), loads):
        load.wait()
        rows = dot(perm[0:half, :], hv[:, d + c:d + c + chunk]).astype(BF)
        hv[far, c:c + chunk] = rows
        xv[own, c:c + chunk] = rows[3 * cap:, :]
    sel = dot_nt(perm[...], pick).astype(BF)
    sels[...] = sel[0:half, :]
    selv[3 * cap:toks, :] = sel[3 * cap:, :]
    backv[...] = place.T.astype(BF)
    a_copy(2, 2).start()
    issue(1)

    pl.semaphore_wait(barrier, 3)
    moves = []
    for off in (2, 3, 1):
        rows = pl.ds((off - 1) * cap, cap)
        for src, dst, snd, rcv in ((sels.at[rows], selv, sr_send, sr_recv), (hv.at[rows, pl.ds(0, d)], xv, xr_send, xr_recv)):
            m = pltpu.make_async_remote_copy(
                src_ref=src, dst_ref=dst.at[rows], send_sem=snd.at[off - 1], recv_sem=rcv.at[off - 1],
                device_id={"data": peer_of(me, off)}, device_id_type=MESH)
            m.start()
            moves.append(m)
    keep_back = pltpu.make_async_copy(backv, back, b_sem)
    keep_back.start()
    for c in range(0, d, chunk):
        xv[near, c:c + chunk] = dot(perm[half:toks, :], hv[:, d + c:d + c + chunk]).astype(BF)

    def mask(rows, first):
        row = lax.broadcasted_iota(jnp.int32, (128, 256), 0)
        col = lax.broadcasted_iota(jnp.int32, (128, 256), 1)
        spread = (row == first // 64 + col // 64).astype(BF)
        return dot(selv[rows, :], spread).astype(BF)

    def low_x(rows, slot, dst, first):
        low = dot_nt(xv[rows, :], abuf[slot]).astype(BF)
        dst[rows, first:first + 256] = low * mask(rows, first)

    lowacc_h[...] = jnp.zeros_like(lowacc_h)
    lowacc_c[...] = jnp.zeros_like(lowacc_c)
    a_copy(0, 0).wait()
    low_x(near, 0, lowg, 0)
    a_copy(1, 1).wait()
    low_x(near, 1, lowu, 0)

    def delta(low, b):
        return (scale * dot(low, b)).astype(BF).astype(F32)

    def hidden(rows, blk, slot, k):
        g = dot(xv[rows, :], wbuf[slot, 0:d]) + delta(lowg[rows, 0:k], lbuf[slot, 0, 0:k])
        u = dot(xv[rows, :], wbuf[slot, d:2 * d]) + delta(lowu[rows, 0:k], lbuf[slot, 1, 0:k])
        hv[rows, cols(blk)] = (jax.nn.silu(g) * u).astype(BF)

    def early(t, carry):
        slot = t % SLOTS
        issue(t + 2)
        for c in gu_copies(t, slot, False):
            c.wait()
        hidden(near, t, slot, kh)
        return carry

    lax.fori_loop(0, EARLY, early, 0)

    keep_back.wait()
    for m in moves:
        m.wait()
    for i in range(10):
        slot = i % 3
        if i >= 2:
            a_copy(i, slot).wait()
        dst = lowg if i == 0 or 2 <= i < 6 else lowu
        first = 0 if i < 2 else 256 * (1 + (i - 2) % 4)
        low_x(far, slot, dst, first)
        if i + 3 < 10:
            a_copy(i + 3, slot).start()

    def group(j, carry):
        def both(r, carry):
            t = EARLY + 3 * j + r
            slot = t % SLOTS
            blk = EARLY + 2 * j + r
            issue(t + 2)
            for c in gu_copies(blk, slot, True):
                c.wait()
            hidden(near, blk, slot, kh)
            hidden(far, blk, slot, kk)
            return carry

        lax.fori_loop(0, 2, both, 0)
        t = EARLY + 3 * j + 2
        slot = t % SLOTS
        issue(t + 2)
        for c in gu_copies(j, slot, True):
            c.wait()
        hidden(far, j, slot, kk)
        return carry

    lax.fori_loop(0, EARLY, group, 0)

    def low_h(i, carry):
        t = n_gu + i
        slot = t % SLOTS
        issue(t + 2)
        for c in ad_copies(i, slot):
            c.wait()
        first = i * per
        hot_sum, cold_sum = lowacc_h[...], lowacc_c[...]
        for q in range(per):
            c = cols(first + q)
            hot_sum += dot_nt(hv[:, c], wbuf[slot, q * kk:q * kk + kh])
            cold_sum += dot_nt(hv[far, c], wbuf[slot, q * kk + kh:(q + 1) * kk])
        lowacc_h[...] = hot_sum
        lowacc_c[...] = cold_sum
        return carry

    lax.fori_loop(0, AD_STEPS, low_h, 0)

    lowd = lowg
    for i in range(kk // 256):
        part = slice(256 * i, 256 * (i + 1))
        if i == 0:
            lowd[near, part] = lowacc_h[near, :].astype(BF) * mask(near, 0)
            lowd[far, part] = lowacc_h[far, :].astype(BF) * mask(far, 0)
        else:
            lowd[far, part] = lowacc_c[:, 256 * (i - 1):256 * i].astype(BF) * mask(far, 256 * i)

    def back_copies(blk):
        p = blk % 2
        c = cols(blk)
        out = []
        for off in (2, 3, 1):
            rows = pl.ds((off - 1) * cap, cap)
            out.append(pltpu.make_async_remote_copy(
                src_ref=ybuf.at[p, rows], dst_ref=ys.at[rows, c], send_sem=y_send.at[p, off - 1],
                recv_sem=y_recv.at[off - 1], device_id={"data": peer_of(me, off)}, device_id_type=MESH))
        mine = pl.ds(3 * cap, toks - 3 * cap)
        return out, pltpu.make_async_copy(ybuf.at[p, mine], ys.at[mine, c], y_sem.at[p])

    def send_back(blk):
        remote, local = back_copies(blk)
        for m in remote:
            m.start()
        local.start()

    def sent(blk):
        remote, local = back_copies(blk)
        for m in remote:
            m.wait_send()
        local.wait()

    def down_rows(i, slot, first, count, k):
        rows = pl.ds(first, count)
        y = dot(hv[rows, :], wbuf[slot]) + delta(lowd[rows, 0:k], lbuf[slot, 0, 0:k])
        ybuf[i % 2, rows, :] = (xv[rows, cols(i)].astype(F32) + y).astype(BF)

    def down(i, carry):
        t = n_ad + i
        slot = t % SLOTS

        @pl.when(i > 0)
        def _():
            send_back(i - 1)

        @pl.when(i > 1)
        def _():
            sent(i - 2)

        issue(t + 2)
        for c in d_copies(i, slot):
            c.wait()
        down_rows(i, slot, half, half, kh)
        down_rows(i, slot, 0, half, kk)
        return carry

    last = dblocks - 1
    lax.fori_loop(0, last, down, 0)
    slot = (n_ad + last) % SLOTS
    send_back(last - 1)
    sent(last - 2)
    for c in d_copies(last, slot):
        c.wait()
    down_rows(last, slot, 0, half, kk)
    down_rows(last, slot, half, half // 2, kh)
    remote, local = back_copies(last)
    for m in remote:
        m.start()
    down_rows(last, slot, half + half // 2, half // 2, kh)
    local.start()
    sent(last - 1)
    sent(last)
    for off in (2, 3, 1):
        rows = pl.ds((off - 1) * cap, cap)
        pltpu.make_async_remote_copy(
            src_ref=ys.at[rows], dst_ref=ys.at[rows], send_sem=y_send.at[0, off - 1], recv_sem=y_recv.at[off - 1],
            device_id={"data": peer_of(me, off)}, device_id_type=MESH).wait_recv()


def mlp(scale, cap, n_local, hot_ids, ids, x, ws, cold, hot):
    toks, d = x.shape
    f = ws[0].shape[1]
    kh, kc = hot[0].shape[0], cold[0].shape[0]
    kk = kh + kc
    half = toks // 2
    pairs = [m for h, c in zip(hot, cold) for m in (h, c)]
    dma = pltpu.SemaphoreType.DMA
    return pl.pallas_call(
        functools.partial(mlp_kernel, scale, cap, n_local),
        in_specs=[pl.BlockSpec(memory_space=pltpu.SMEM), pl.BlockSpec(memory_space=pltpu.VMEM)] + [pl.BlockSpec(memory_space=pl.ANY)] * 16,
        out_specs=[pl.BlockSpec(memory_space=pl.ANY)] * 2,
        out_shape=[jax.ShapeDtypeStruct((toks, d), BF), jax.ShapeDtypeStruct((toks, toks), BF)],
        scratch_shapes=[
            pltpu.VMEM((toks, d), BF),
            pltpu.VMEM((toks, 128), BF),
            pltpu.VMEM((half, 128), BF),
            pltpu.VMEM((toks, toks), BF),
            pltpu.VMEM((toks, toks), BF),
            pltpu.VMEM((toks, f), BF),
            pltpu.VMEM((SLOTS, f, FB), BF),
            pltpu.VMEM((SLOTS, 2, kk, FB), BF),
            pltpu.VMEM((3, 256, d), BF),
            pltpu.VMEM((toks, kk), BF),
            pltpu.VMEM((toks, kk), BF),
            pltpu.VMEM((toks, kh), F32),
            pltpu.VMEM((half, kc), F32),
            pltpu.VMEM((2, toks, FB), BF),
            dma((d // 1024,)), dma, dma((3,)), dma((3,)), dma((3,)), dma((3,)),
            dma((SLOTS, 2)), dma((SLOTS, 4)), dma((SLOTS, 2 * (f // FB // AD_STEPS))), dma((3,)), dma((2, 3)), dma((3,)), dma((2,)),
        ],
        compiler_params=pltpu.CompilerParams(
            collective_id=0, has_side_effects=True, vmem_limit_bytes=63 * 1024 * 1024),
    )(hot_ids, ids.reshape(1, toks), x, *ws, *pairs)


def solution(mesh):
    group = mesh.shape["data"]
    token_spec = P(("replica", "data"), None)
    store_spec = P("data", None, None)
    full_mat = P(None, None)
    full_set = P(None, None, None)
    in_specs = (token_spec, P(("replica", "data")), full_mat, full_mat, full_mat) + (store_spec,) * 6 + (P(None),) + (full_set,) * 6

    def device_step(x, adapter_id, w_gate, w_up, w_down, a_gate, b_gate, a_up, b_up, a_down, b_down, hot_ids, hot_a_gate, hot_b_gate, hot_a_up, hot_b_up, hot_a_down, hot_b_down):
        cap = x.shape[0] // (2 * group)
        scale = LORA_ALPHA / a_gate.shape[2]

        def flat_a(a):
            return jnp.swapaxes(a, 1, 2).reshape(-1, a.shape[1])

        def flat_b(b):
            return b.reshape(-1, b.shape[2])

        cold = [flat_a(a_gate), flat_b(b_gate), flat_a(a_up), flat_b(b_up), flat_a(a_down), flat_b(b_down)]
        hot = [flat_a(hot_a_gate), flat_b(hot_b_gate), flat_a(hot_a_up), flat_b(hot_b_up), flat_a(hot_a_down), flat_b(hot_b_down)]
        ys, back = mlp(scale, cap, a_gate.shape[0], hot_ids, adapter_id, x, (w_gate, w_up, w_down), cold, hot)
        return unroute(back, ys)

    return jax.shard_map(device_step, mesh=mesh, in_specs=in_specs, out_specs=token_spec, check_vma=False)
```
